32 devices in a mesh: groups: 2 (over x), dev: 16 (over z, y, core).
Axes of the slice: x: 2, y: 2, z: 4, core: 2. Of those that a mesh axis runs over, the one named last changes fastest.
Arguments:
- queries: bfloat16 [32, 512, 512], P(('groups', 'dev')), parts along dimension 0, may hold values from -120 to 120
- key_values: bfloat16 [2, 32, 512, 128], P(None, ('groups', 'dev')), parts along dimension 1, may hold values from -4 to 4
- lengths: int32 [4], P('groups'), parts along dimension 0, may hold values from 1 to 512, as said below
- out_proj: bfloat16 [4096, 2048], P('dev'), may hold values from -0.09375 to 0.09375
- residual: bfloat16 [32, 64, 2048], P(('groups', 'dev')), parts along dimension 0, may hold values from -8 to 8
- norm_gain: bfloat16 [2048], replicated, may hold values from 0.25 to 1.75
- router: bfloat16 [2048, 16], replicated, may hold values from -0.125 to 0.125
- expert_ids: int32 [32, 64, 8], P(('groups', 'dev')), parts along dimension 0, may hold values from 0 to 15, all different within a row; in each aligned block of 64 rows (0 to 63, 64 to 127, ..., all dimensions but the last counted through in order) at most 48 rows name the same one
- expert_gate_up: bfloat16 [16, 2048, 1536], P('dev'), may hold values from -0.125 to 0.125
- expert_down: bfloat16 [16, 768, 2048], P('dev'), may hold values from -0.21875 to 0.21875
Outputs:
- output: bfloat16 [32, 64, 2048], P(('groups', 'dev')), parts along dimension 0
The draws below stay inside these ranges and needn't reach their ends.
There are 2 independent parts, one for each index of `groups`. The reference program is written for one: setup_inputs(seed, part) draws one part's arguments, and reference() takes and returns one part's arrays. A program takes and returns all parts, laid end to end along the dimension named above; an argument that names none is the same for every part. Nothing has to cross between parts.
Inputs may be any that keep to these rules, and one draw needn't show every extreme that they name: `lengths`: in every draw some request has all 512 cache slots filled. Each token names 8 different experts. The tokens of one block of expert_ids name any one expert at most 48 times, and in every draw some block names some expert exactly 48 times.
All inputs are finite; a program needn't handle non-finite values.
Results may differ from the reference program's by a relative error of at most 0.011.
Values may be sent and summed in bfloat16 or wider, within the bound.
A program may use at most 128 MiB of HBM per device.

```python
import math
import jax
import jax.numpy as jnp
import numpy as np
from jax import lax

D = 2048
HEADS = 32
KV_HEADS = 4
HEAD_DIM = 128
FF = 768
TOP = 8
TOK_DEV = 64
CTX = 512
GROUP = 8
QH = 4
REQS = 2
SPAN = 512
HALF = 512
EXPERTS = 16
CAP = 48


def attention_pair(key):
    base_key = jax.random.fold_in(key, 101)
    key_query, key_pairs = jax.random.split(base_key, 2)
    block_count = GROUP * REQS
    kv_draw = jnp.clip(jax.random.normal(key_pairs, (2, block_count, HALF, HEAD_DIM), jnp.float32), -4.0, 4.0)
    query_draw = jnp.clip(2.0 * jax.random.normal(key_query, (block_count, SPAN, QH * HEAD_DIM), jnp.float32), -8.0, 8.0)
    return (query_draw, kv_draw)


def draw_queries(key, part):
    return attention_pair(key)[0].astype(jnp.bfloat16)


def draw_key_values(key, part):
    return attention_pair(key)[1].astype(jnp.bfloat16)


def draw_lengths(key, part):
    base_key = jax.random.fold_in(key, 202)
    key_len, key_full = jax.random.split(base_key)
    drawn_len = jax.random.randint(key_len, (REQS,), 1, CTX)
    filled = jax.random.randint(key_full, (), 0, REQS)
    return jnp.where(jnp.arange(REQS) == filled, CTX, drawn_len).astype(jnp.int32)


def draw_residual(key, part):
    base_key = jax.random.fold_in(key, 303)
    key_noise = jax.random.fold_in(base_key, 0)
    noise_part = jax.random.normal(key_noise, (GROUP * REQS, TOK_DEV, D), jnp.float32)
    drawn_value = 0.25 * noise_part
    return jnp.clip(drawn_value, -8.0, 8.0).astype(jnp.bfloat16)


def steps_of(stream_key, dims, cuts, least, high):
    gain = 1.0
    for position, shards_of in cuts:
        steps = jax.random.uniform(jax.random.fold_in(jax.random.fold_in(stream_key, 6), position), (shards_of,), jnp.float32, least / len(cuts), high / len(cuts))
        gain = gain * jnp.repeat(jnp.exp(steps), dims[position] // shards_of).reshape((-1,) + (1,) * (len(dims) - 1 - position))
    return gain


def routed_block(stream_key, own, number, rows, amount, top, reach, slope):
    sequence = jax.random.permutation(stream_key, amount)
    packed, usual = load_shares(amount, rows * top, reach, slope, True), load_shares(amount, rows * top, reach, slope, False)
    places = jnp.arange(amount)

    def named(sizes, offset_by):
        used = int((sizes > 0).sum())
        fixed = max(1, used // 4)
        moved = fixed + (places - fixed + offset_by * (used - fixed)) % max(1, amount - fixed)
        return jnp.zeros((amount,), jnp.int32).at[sequence[jnp.where(places < fixed, places, moved)]].set(jnp.asarray(sizes, jnp.int32))

    sizes = jnp.where(number % 4 == 0, named(packed, number // 4), named(usual, number - number // 4 - 1))
    mixed = jax.random.permutation(jax.random.fold_in(own, 3), amount)
    source_of, taker = mixed[0:amount // 2 * 2:2], mixed[1:amount // 2 * 2:2]
    room = jnp.minimum(sizes[source_of] - 1, reach - sizes[taker]) // 2
    room = jnp.where((source_of == sequence[0]) | (taker == sequence[0]) | (sizes[taker] == 0), 0, jnp.maximum(room, 0))
    moved = jax.random.randint(jax.random.fold_in(own, 4), (amount // 2,), 0, 1 << 20) % (room + 1)
    sizes = sizes.at[source_of].add(-moved).at[taker].add(moved)
    items = jnp.searchsorted(jnp.cumsum(sizes), jnp.arange(rows * top), side="right").astype(jnp.int32)
    listing = items.reshape(top, rows).T
    listing = listing[jax.random.permutation(jax.random.fold_in(own, 1), rows)]
    offset_by = jax.random.randint(jax.random.fold_in(own, 2), (rows, 1), 0, top)
    return jnp.take_along_axis(listing, (jnp.arange(top)[None, :] + offset_by) % top, axis=1)


def load_shares(number_of, total, bound, skew, full):
    weights = [(1 << 20) // math.isqrt(standing ** skew) + 1 for standing in range(1, number_of + 1)]
    largest = bound if full else min(bound, max(-(-total // number_of), total * weights[0] // sum(weights)))
    least = 1 if total - largest >= number_of - 1 else 0
    given, spare = [largest] + [least] * (number_of - 1), total - largest - least * (number_of - 1)
    while spare > 0:
        free = [i for i in range(1, number_of) if given[i] < largest] or [i for i in range(1, number_of) if given[i] < bound]
        mass, left = sum([weights[i] for i in free]), spare
        for i in free:
            addition = min(bound - given[i], max(1, left * weights[i] // mass), spare)
            given[i] = given[i] + addition
            spare = spare - addition
    return np.array(given)


def noise(rng, extent, scale, reach, cuts=(), held_as=jnp.bfloat16):
    values = scale * jax.random.normal(rng, extent, jnp.float32)
    if cuts:
        values = values * steps_of(rng, extent, cuts, -0.22, 0.18)
    return jnp.clip(values, -reach, reach).astype(held_as)


def setup_inputs(seed: int = 0, part: int = 0) -> dict:
    arg_keys = jax.random.split(jax.random.key(seed), 11)
    part_splits = jax.random.split(jax.random.fold_in(arg_keys[10], part), 11)
    queries = draw_queries(jax.random.fold_in(jax.random.fold_in(arg_keys[10], part), 71), part)
    key_values = draw_key_values(jax.random.fold_in(jax.random.fold_in(arg_keys[10], part), 71), part)
    lengths = draw_lengths(jax.random.fold_in(jax.random.fold_in(arg_keys[10], part), 71), part)
    out_proj = noise(arg_keys[3], (HEADS * HEAD_DIM, D), (HEADS * HEAD_DIM) ** -0.5, 0.09375, ((0, 16),))
    residual = draw_residual(jax.random.fold_in(jax.random.fold_in(arg_keys[10], part), 71), part)
    norm_gain = jnp.clip(1.0 + 0.15 * jax.random.normal(arg_keys[5], (D,), jnp.float32), 0.25, 1.75).astype(jnp.bfloat16)
    router = noise(arg_keys[6], (D, EXPERTS), D ** -0.5, 0.125)
    expert_ids_keys = jax.random.split(jax.random.fold_in(part_splits[7], 1), (GROUP * REQS) * TOK_DEV // TOK_DEV)
    expert_ids_turns = jax.random.permutation(jax.random.fold_in(part_splits[7], 3), (GROUP * REQS) * TOK_DEV // TOK_DEV)
    expert_ids = jax.vmap(lambda own, number: routed_block(jax.random.fold_in(part_splits[7], 2), own, number, TOK_DEV, EXPERTS, TOP, CAP, 2))(expert_ids_keys, expert_ids_turns).reshape((GROUP * REQS, TOK_DEV, TOP))
    expert_gate_up = noise(arg_keys[8], (EXPERTS, D, 2 * FF), D ** -0.5, 0.125, ((0, 16),))
    expert_down = noise(arg_keys[9], (EXPERTS, FF, D), FF ** -0.5, 0.21875, ((0, 16),))
    return dict(queries=queries, key_values=key_values, lengths=lengths, out_proj=out_proj, residual=residual, norm_gain=norm_gain, router=router, expert_ids=expert_ids, expert_gate_up=expert_gate_up, expert_down=expert_down)


EPSILON = 1e-06

def route_slots(flat_ids):
    expert_marks = (flat_ids.reshape(-1)[:, None] == jnp.arange(EXPERTS, dtype=jnp.int32)[None, :]).astype(jnp.int32)
    before = jnp.cumsum(expert_marks, axis=0) - expert_marks
    return lax.optimization_barrier(jnp.sum(before * expert_marks, axis=1)).reshape(flat_ids.shape)

def slot_rows(flat_ids, slot_index):
    positions = (flat_ids * CAP + slot_index).reshape(-1).astype(jnp.int32)
    tokens = jnp.repeat(jnp.arange(TOK_DEV, dtype=jnp.int32), TOP)
    return jnp.full((EXPERTS * CAP,), -1, jnp.int32).at[positions].set(tokens)

def expert_rows(gathered, gate_up, down_proj):
    projected = jnp.dot(gathered, gate_up, preferred_element_type=jnp.float32)
    activation = (jax.nn.silu(projected[:, :FF]) * projected[:, FF:]).astype(jnp.bfloat16)
    return jnp.dot(activation, down_proj, preferred_element_type=jnp.float32).astype(jnp.bfloat16)

def reference(queries, key_values, lengths, out_proj, residual, norm_gain, router, expert_ids, expert_gate_up, expert_down):
    block_count = GROUP * REQS
    score_scale = 1.0 / math.sqrt(HEAD_DIM)
    kv_seq = key_values.reshape(2, KV_HEADS, 2, REQS, HALF, HEAD_DIM).transpose(0, 1, 3, 2, 4, 5)
    kv_seq = kv_seq.reshape(2, KV_HEADS, REQS, 2 * HALF, HEAD_DIM)
    query_blocks = queries.reshape(block_count, SPAN, QH, HEAD_DIM)
    positions = jnp.arange(CTX + SPAN, dtype=jnp.int32)
    row_ids = jnp.arange(SPAN, dtype=jnp.int32)
    rank_ids = jnp.arange(block_count, dtype=jnp.int32) // REQS
    requests = jnp.arange(block_count, dtype=jnp.int32) % REQS

    def attend(element):
        rank_no, request, block_q = element
        key_rows = kv_seq[0, rank_no // 2, request]
        value_rows = kv_seq[1, rank_no // 2, request]
        scores = jnp.einsum('tjd,pd->jtp', block_q.astype(jnp.float32), key_rows.astype(jnp.float32)) * score_scale
        visible = (positions[None, :] < lengths[request]) | (positions[None, :] >= CTX) & (positions[None, :] - CTX <= row_ids[:, None])
        scores = jnp.where(visible[None], scores, -jnp.inf)
        row_max = lax.optimization_barrier(jnp.max(scores, axis=-1, keepdims=True))
        raised = jnp.exp(scores - row_max)
        weights = (raised / lax.optimization_barrier(jnp.sum(raised, axis=-1, keepdims=True))).astype(jnp.bfloat16)
        mixture = jnp.einsum('jtp,pd->tjd', weights.astype(jnp.float32), value_rows.astype(jnp.float32))
        return mixture.astype(jnp.bfloat16)
    head_out = lax.map(attend, (rank_ids, requests, query_blocks))
    head_out = head_out.reshape(GROUP, REQS, SPAN, QH * HEAD_DIM).transpose(1, 2, 0, 3).reshape(REQS * SPAN, HEADS * HEAD_DIM)
    attended = jnp.dot(head_out, out_proj, preferred_element_type=jnp.float32)
    attended = attended.reshape(REQS, GROUP, TOK_DEV, D).transpose(1, 0, 2, 3).reshape(block_count, TOK_DEV, D)
    stream = (residual.astype(jnp.float32) + attended).astype(jnp.bfloat16)
    values = stream.astype(jnp.float32)
    normed = (values * lax.rsqrt(lax.optimization_barrier(jnp.mean(values * values, axis=-1, keepdims=True)) + EPSILON) * norm_gain.astype(jnp.float32)).astype(jnp.bfloat16)
    logits = jnp.dot(normed.reshape(block_count * TOK_DEV, D), router, preferred_element_type=jnp.float32).reshape(block_count, TOK_DEV, EXPERTS)
    onehot = expert_ids[..., None] == jnp.arange(EXPERTS, dtype=jnp.int32)
    chosen = lax.optimization_barrier(jnp.sum(jnp.where(onehot, logits[:, :, None, :], 0.0), axis=-1))
    raised_gate = jnp.exp(chosen)
    gate_weights = raised_gate / lax.optimization_barrier(jnp.sum(raised_gate, axis=-1, keepdims=True))
    slots = jax.vmap(route_slots)(expert_ids)
    slot_table = jax.vmap(slot_rows)(expert_ids, slots)

    def visit(summed, element):
        gate_up, down_proj, expert = element
        token_pick = lax.dynamic_slice_in_dim(slot_table, (expert * CAP).astype(jnp.int32), CAP, axis=1)
        gathered = jnp.take_along_axis(normed, jnp.maximum(token_pick, 0)[:, :, None], axis=1)
        outputs = expert_rows(gathered.reshape(block_count * CAP, D), gate_up, down_proj).reshape(block_count, CAP, D)
        is_chosen = expert_ids == expert
        weight = lax.optimization_barrier(jnp.sum(jnp.where(is_chosen, gate_weights, 0.0), axis=2))
        slot_pick = lax.optimization_barrier(jnp.sum(jnp.where(is_chosen, slots, 0), axis=2)).astype(jnp.int32)
        picked = jnp.take_along_axis(outputs, slot_pick[:, :, None], axis=1)
        return (summed + weight[:, :, None] * picked.astype(jnp.float32), None)
    summed, _ = lax.scan(visit, jnp.zeros((block_count, TOK_DEV, D), jnp.float32), (expert_gate_up, expert_down, jnp.arange(EXPERTS, dtype=jnp.int32)))
    return (values + summed).astype(jnp.bfloat16)
```

```python
import functools
import math

import jax
import jax.numpy as jnp
from jax import lax
from jax.experimental import pallas as pl
from jax.experimental.pallas import tpu as pltpu
from jax.sharding import PartitionSpec as P

HEAD_DIM = 128
FF = 768
TOP = 8
TOK_DEV = 64
CTX = 512
GROUP = 8
QH = 4
SPAN = 512
EPSILON = 1e-06
MESH = pl.DeviceIdType.MESH


def bit_count(number):
    return number.bit_length() - 1


def flipped(index, bits):
    for bit in bits:
        index = index + (1 - 2 * ((index // (1 << bit)) % 2)) * (1 << bit)
    return index


def subset(bits, number):
    return [bit for place, bit in enumerate(bits) if number >> place & 1]


def greet(me, bits):
    barrier = pltpu.get_barrier_semaphore()
    for bit in bits:
        pl.semaphore_signal(
            barrier, inc=1, device_id={"dev": flipped(me, [bit])}, device_id_type=MESH
        )
    pl.semaphore_wait(barrier, len(bits))


def scatter_steps(me, unit, part_no, order, cols, x_ref, recv, stage, send_sem, recv_sem, block_of):
    k = len(order)
    total = (1 << k) - 1
    first = [total - ((1 << (k - s)) - 1) for s in range(k)]

    def arrived(step, number):
        return pltpu.make_async_remote_copy(
            src_ref=recv.at[first[step] + number, :, cols],
            dst_ref=recv.at[first[step] + number, :, cols],
            send_sem=send_sem.at[part_no, first[step] + number],
            recv_sem=recv_sem.at[part_no, first[step] + number],
            device_id={"dev": flipped(me, [unit + order[step]])},
            device_id_type=MESH,
        )

    copies = []

    def send(step):
        for number in range(1 << (k - 1 - step)):
            slot = first[step] + number
            flips = [order[step]] + subset(order[step + 1 :], number)
            block = block_of(flips)
            if step == 0:
                source = x_ref.at[block, :, cols]
            else:
                value = x_ref[block, :, cols].astype(jnp.float32)
                for earlier in range(step):
                    place = (1 << (step - earlier - 1)) + (number << (step - earlier))
                    arrived(earlier, place).wait_recv()
                    value = value + recv[first[earlier] + place, :, cols].astype(jnp.float32)
                spot = slot - first[1]
                stage[spot, :, cols] = value.astype(stage.dtype)
                source = stage.at[spot, :, cols]
            copy = pltpu.make_async_remote_copy(
                src_ref=source,
                dst_ref=recv.at[slot, :, cols],
                send_sem=send_sem.at[part_no, slot],
                recv_sem=recv_sem.at[part_no, slot],
                device_id={"dev": flipped(me, [unit + order[step]])},
                device_id_type=MESH,
            )
            copy.start()
            copies.append(copy)

    def finish(o_ref):
        value = x_ref[block_of([]), :, cols].astype(jnp.float32)
        for earlier in range(k):
            arrived(earlier, 0).wait_recv()
            value = value + recv[first[earlier], :, cols].astype(jnp.float32)
        o_ref[:, cols] = value
        for copy in copies:
            copy.wait_send()

    return send, finish


def scatter_kernel(unit, parts, bits, x_ref, o_ref, recv, stage, send_sem, recv_sem):
    me = lax.axis_index("dev")
    greet(me, [unit + bit for bit in bits])
    rank = me // (1 << unit)
    runs = [
        scatter_steps(
            me, unit, number, order, cols, x_ref, recv, stage, send_sem, recv_sem,
            lambda flips: flipped(rank, flips),
        )
        for number, (order, cols) in enumerate(parts)
    ]
    for step in range(len(bits)):
        for send, _ in runs:
            send(step)
    for _, finish in runs:
        finish(o_ref)


def reduce_scatter(x, unit, orders, collective_id):
    blocks, rows, width = x.shape
    bits = sorted(orders[0])
    cut = width * 3 // 4 // 128 * 128
    parts = [(orders[0], pl.ds(0, cut)), (orders[1], pl.ds(cut, width - cut))]
    return pl.pallas_call(
        functools.partial(scatter_kernel, unit, parts, bits),
        out_shape=jax.ShapeDtypeStruct((rows, width), jnp.float32),
        in_specs=[pl.BlockSpec(memory_space=pltpu.VMEM)],
        out_specs=pl.BlockSpec(memory_space=pltpu.VMEM),
        scratch_shapes=[
            pltpu.VMEM((blocks - 1, rows, width), x.dtype),
            pltpu.VMEM((max(blocks // 2 - 1, 1), rows, width), x.dtype),
            pltpu.SemaphoreType.DMA((2, blocks - 1)),
            pltpu.SemaphoreType.DMA((2, blocks - 1)),
        ],
        compiler_params=pltpu.CompilerParams(collective_id=collective_id, has_side_effects=True),
    )(x)


def gather_kernel(parts, bits, x_ref, g_ref, ox_ref, og_ref, send_sem, recv_sem, own_sem):
    me = lax.axis_index("dev")
    greet(me, bits)
    k = len(bits)
    pairs = [(x_ref, ox_ref), (g_ref, og_ref)]
    local = []
    for number, (source, target) in enumerate(pairs):
        copy = pltpu.make_async_copy(source, target.at[me], own_sem.at[number])
        copy.start()
        local.append(copy)
    sent = []

    def forward(part_no, held, step):
        which, order, cols = parts[part_no]
        source, target = pairs[which]
        block = flipped(me, subset(order, held))
        slot = (1 << step) - 1 + held
        copy = pltpu.make_async_remote_copy(
            src_ref=source.at[:, cols] if held == 0 else target.at[block, :, cols],
            dst_ref=target.at[block, :, cols],
            send_sem=send_sem.at[part_no, slot],
            recv_sem=recv_sem.at[part_no, slot],
            device_id={"dev": flipped(me, [order[step]])},
            device_id_type=MESH,
        )
        copy.start()
        sent.append(copy)

    def arrive(part_no, held, step):
        which, order, cols = parts[part_no]
        target = pairs[which][1]
        block = flipped(me, subset(order, held) + [order[step]])
        slot = (1 << step) - 1 + held
        pltpu.make_async_remote_copy(
            src_ref=target.at[block, :, cols],
            dst_ref=target.at[block, :, cols],
            send_sem=send_sem.at[part_no, slot],
            recv_sem=recv_sem.at[part_no, slot],
            device_id={"dev": flipped(me, [order[step]])},
            device_id_type=MESH,
        ).wait_recv()

    for step in range(k):
        for part_no in range(len(parts)):
            forward(part_no, 0, step)
    for step in range(k):
        for held in range(1 << step):
            for part_no in range(len(parts)):
                arrive(part_no, held, step)
                for later in range(step + 1, k):
                    forward(part_no, held + (1 << step), later)
    for copy in local:
        copy.wait()
    for copy in sent:
        copy.wait_send()


def all_gather(x, gates, orders, collective_id):
    rows, width = x.shape
    bits = sorted(orders[0])
    count = 1 << len(bits)
    cut = width * 3 // 4 // 128 * 128
    parts = [
        (1, orders[0], pl.ds(0, gates.shape[1])),
        (0, orders[0], pl.ds(0, cut)),
        (0, orders[1], pl.ds(cut, width - cut)),
    ]
    return pl.pallas_call(
        functools.partial(gather_kernel, parts, bits),
        out_shape=[
            jax.ShapeDtypeStruct((count, rows, width), x.dtype),
            jax.ShapeDtypeStruct((count,) + gates.shape, gates.dtype),
        ],
        in_specs=[pl.BlockSpec(memory_space=pltpu.VMEM)] * 2,
        out_specs=[pl.BlockSpec(memory_space=pltpu.VMEM)] * 2,
        scratch_shapes=[
            pltpu.SemaphoreType.DMA((3, count - 1)),
            pltpu.SemaphoreType.DMA((3, count - 1)),
            pltpu.SemaphoreType.DMA((2,)),
        ],
        compiler_params=pltpu.CompilerParams(collective_id=collective_id, has_side_effects=True),
    )(x, gates)


def swapped(order, one, two):
    order = list(order)
    order[one], order[two] = order[two], order[one]
    return order


def partner(block, axis, stride):
    count = lax.axis_size(axis)
    route = [(i, i ^ 1 << stride) for i in range(count)]
    return lax.ppermute(block, axis, route)


def per_device(
    queries,
    key_values,
    lengths,
    out_proj,
    residual,
    norm_gain,
    router,
    expert_ids,
    expert_gate_up,
    expert_down,
):
    devices = lax.axis_size("dev")
    my_index = lax.axis_index("dev")
    width = residual.shape[-1]
    requests_n = devices // GROUP
    low_bits = bit_count(requests_n)
    tp_rank = my_index // requests_n
    request = my_index % requests_n
    is_upper = tp_rank % 2 == 1
    own_half = key_values[:, 0]
    other_half = partner(own_half, "dev", low_bits)
    first_part = jnp.where(is_upper, other_half, own_half)
    second_part = jnp.where(is_upper, own_half, other_half)
    key_seq = jnp.concatenate([first_part, second_part], axis=1)
    length = lengths[request]
    positions = jnp.arange(CTX + SPAN, dtype=jnp.int32)
    qblock = math.gcd(SPAN, 256)
    score_scale = 1.0 / math.sqrt(HEAD_DIM)
    block_queries = queries[0].reshape(SPAN // qblock, qblock, QH, HEAD_DIM)
    starts = jnp.arange(SPAN // qblock, dtype=jnp.int32) * qblock

    def attend(element):
        block_q, start = element
        scores = (
            jnp.einsum("tjd,pd->jtp", block_q, key_seq[0], preferred_element_type=jnp.float32)
            * score_scale
        )
        row_ids = start + jnp.arange(qblock, dtype=jnp.int32)
        visible = (positions[None, :] < length) | (positions[None, :] >= CTX) & (
            positions[None, :] - CTX <= row_ids[:, None]
        )
        scores = jnp.where(visible[None], scores, -jnp.inf)
        row_max = jnp.max(scores, axis=-1, keepdims=True)
        raised = jnp.exp(scores - row_max)
        weights = (raised / jnp.sum(raised, axis=-1, keepdims=True)).astype(jnp.bfloat16)
        mixture = jnp.einsum("jtp,pd->tjd", weights, key_seq[1], preferred_element_type=jnp.float32)
        return mixture.astype(jnp.bfloat16)

    head_out = lax.map(attend, (block_queries, starts)).reshape(SPAN, QH * HEAD_DIM)
    proj_block = out_proj
    for bit_no in range(low_bits):
        arrived = partner(proj_block, "dev", bit_no)
        is_high = my_index >> bit_no & 1 == 1
        proj_block = jnp.where(
            is_high,
            jnp.concatenate([arrived, proj_block], axis=0),
            jnp.concatenate([proj_block, arrived], axis=0),
        )
    partial_value = jnp.dot(head_out, proj_block, preferred_element_type=jnp.float32)
    pieces = partial_value.astype(jnp.bfloat16).reshape(GROUP, TOK_DEV, width)
    near = list(range(bit_count(GROUP)))
    attended = reduce_scatter(pieces, low_bits, [near, swapped(near, 0, 1)], 1)
    stream = (residual[0].astype(jnp.float32) + attended).astype(jnp.bfloat16)
    values = stream.astype(jnp.float32)
    normed = (
        values
        * lax.rsqrt(jnp.mean(values * values, axis=-1, keepdims=True) + EPSILON)
        * norm_gain.astype(jnp.float32)
    ).astype(jnp.bfloat16)
    logits = jnp.dot(normed, router, preferred_element_type=jnp.float32)
    experts_n = router.shape[1]
    token_ids = expert_ids[0]
    named = jnp.any(token_ids[..., None] == jnp.arange(experts_n, dtype=jnp.int32), axis=1)
    raised_gate = jnp.where(named, jnp.exp(logits), 0.0)
    gates = raised_gate / jnp.sum(raised_gate, axis=-1, keepdims=True)
    lanes = -(-TOK_DEV // 128) * 128
    gates = jnp.pad(gates.T, ((0, 0), (0, lanes - TOK_DEV)))
    every = list(range(bit_count(devices)))
    far = every[::-1]
    count = len(far)
    rows_all, gates_all = all_gather(normed, gates, [far, swapped(far, count - 3, count - 2)], 2)
    my_gates = lax.dynamic_index_in_dim(gates_all, my_index, 1, keepdims=False)[:, :TOK_DEV]
    flat_rows = rows_all.reshape(devices * TOK_DEV, width)
    projected = jnp.dot(flat_rows, expert_gate_up[0], preferred_element_type=jnp.float32)
    activation = (jax.nn.silu(projected[:, :FF]) * projected[:, FF:]).astype(jnp.bfloat16)
    produced = jnp.dot(activation, expert_down[0], preferred_element_type=jnp.float32)
    weighted = (my_gates.reshape(-1, 1) * produced).astype(jnp.bfloat16)
    weighted = weighted.reshape(devices, TOK_DEV, width)
    combined = reduce_scatter(weighted, 0, [every, swapped(every, 1, 2)], 3)
    return (values + combined).astype(jnp.bfloat16)[None]


def solution(mesh):
    return jax.shard_map(
        per_device,
        mesh=mesh,
        in_specs=(
            P(("groups", "dev"), None, None),
            P(None, ("groups", "dev"), None, None),
            P("groups"),
            P("dev", None),
            P(("groups", "dev"), None, None),
            P(),
            P(),
            P(("groups", "dev"), None, None),
            P("dev", None, None),
            P("dev", None, None),
        ),
        out_specs=P(("groups", "dev"), None, None),
        check_vma=False,
    )
```

```python
import functools
import math

import jax
import jax.numpy as jnp
from jax import lax
from jax.experimental import pallas as pl
from jax.experimental.pallas import tpu as pltpu
from jax.sharding import PartitionSpec as P

HEAD_DIM = 128
FF = 768
TOK_DEV = 64
GROUP = 8
EPSILON = 1e-06
MESH = pl.DeviceIdType.MESH


def bit_count(number):
    return number.bit_length() - 1


def flipped(index, bits):
    for bit in bits:
        index = index + (1 - 2 * ((index // (1 << bit)) % 2)) * (1 << bit)
    return index


def subset(bits, number):
    return [bit for place, bit in enumerate(bits) if number >> place & 1]


def greet(me, bits):
    barrier = pltpu.get_barrier_semaphore()
    for bit in bits:
        pl.semaphore_signal(
            barrier, inc=1, device_id={"dev": flipped(me, [bit])}, device_id_type=MESH
        )
    pl.semaphore_wait(barrier, len(bits))


def scatter_steps(me, unit, part_no, order, cols, x_ref, recv, stage, send_sem, recv_sem, block_of):
    k = len(order)
    total = (1 << k) - 1
    first = [total - ((1 << (k - s)) - 1) for s in range(k)]

    def arrived(step, number):
        return pltpu.make_async_remote_copy(
            src_ref=recv.at[first[step] + number, :, cols],
            dst_ref=recv.at[first[step] + number, :, cols],
            send_sem=send_sem.at[part_no, first[step] + number],
            recv_sem=recv_sem.at[part_no, first[step] + number],
            device_id={"dev": flipped(me, [unit + order[step]])},
            device_id_type=MESH,
        )

    copies = []

    def send(step, only=None):
        for number in reversed(range(1 << (k - 1 - step))) if only is None else [only]:
            slot = first[step] + number
            flips = [order[step]] + subset(order[step + 1 :], number)
            block = block_of(flips)
            if step == 0:
                source = x_ref.at[block, :, cols]
            else:
                value = x_ref[block, :, cols].astype(jnp.float32)
                for earlier in range(step):
                    place = (1 << (step - earlier - 1)) + (number << (step - earlier))
                    arrived(earlier, place).wait_recv()
                    value = value + recv[first[earlier] + place, :, cols].astype(jnp.float32)
                spot = slot - first[1]
                stage[spot, :, cols] = value.astype(stage.dtype)
                source = stage.at[spot, :, cols]
            copy = pltpu.make_async_remote_copy(
                src_ref=source,
                dst_ref=recv.at[slot, :, cols],
                send_sem=send_sem.at[part_no, slot],
                recv_sem=recv_sem.at[part_no, slot],
                device_id={"dev": flipped(me, [unit + order[step]])},
                device_id_type=MESH,
            )
            copy.start()
            copies.append(copy)

    def finish(o_ref):
        value = x_ref[block_of([]), :, cols].astype(jnp.float32)
        for earlier in range(k):
            arrived(earlier, 0).wait_recv()
            value = value + recv[first[earlier], :, cols].astype(jnp.float32)
        o_ref[:, cols] = value
        for copy in copies:
            copy.wait_send()

    return send, finish


def scatter_kernel(unit, parts, bits, x_ref, o_ref, recv, stage, send_sem, recv_sem):
    me = lax.axis_index("dev")
    greet(me, [unit + bit for bit in bits])
    rank = me // (1 << unit)
    runs = [
        scatter_steps(
            me, unit, number, order, cols, x_ref, recv, stage, send_sem, recv_sem,
            lambda flips: flipped(rank, flips),
        )
        for number, (order, cols) in enumerate(parts)
    ]
    for step in range(len(bits)):
        for send, _ in runs:
            send(step)
    for _, finish in runs:
        finish(o_ref)


def attend_block(block, length, q_ref, halves, rows):
    heads = q_ref.shape[1] // HEAD_DIM
    picked = pl.ds(pl.multiple_of(block * rows, rows), rows)
    query = jnp.concatenate(
        [q_ref[picked, head * HEAD_DIM : (head + 1) * HEAD_DIM] for head in range(heads)], axis=0
    )
    scale = 1.0 / math.sqrt(HEAD_DIM)
    contract = (((1,), (1,)), ((), ()))
    old = lax.dot_general(query, halves[0, 0], contract, preferred_element_type=jnp.float32) * scale
    new = lax.dot_general(query, halves[1, 0], contract, preferred_element_type=jnp.float32) * scale
    column = lax.broadcasted_iota(jnp.int32, (1, old.shape[1]), 1)
    old = jnp.where(column < length, old, -1e30)
    column = lax.broadcasted_iota(jnp.int32, (rows, new.shape[1]), 1)
    token = lax.broadcasted_iota(jnp.int32, (rows, new.shape[1]), 0) + block * rows
    bias = jnp.where(column <= token, 0.0, -1e30)
    new = new + jnp.concatenate([bias] * heads, axis=0)
    top = jnp.maximum(jnp.max(old, axis=1, keepdims=True), jnp.max(new, axis=1, keepdims=True))
    old = jnp.exp(old - top)
    new = jnp.exp(new - top)
    total = jnp.sum(old, axis=1, keepdims=True) + jnp.sum(new, axis=1, keepdims=True)
    mixed = jnp.dot(old.astype(jnp.bfloat16), halves[0, 1], preferred_element_type=jnp.float32)
    mixed += jnp.dot(new.astype(jnp.bfloat16), halves[1, 1], preferred_element_type=jnp.float32)
    mixed = (mixed / total).astype(jnp.bfloat16)
    return jnp.concatenate(
        [mixed[head * rows : (head + 1) * rows] for head in range(heads)], axis=1
    )


def attention_kernel(
    unit, parts, bits,
    lengths_ref, q_ref, kv_ref, proj_ref, o_ref,
    halves, proj, heads, x, recv, stage,
    send_sem, recv_sem, kv_sem, proj_send, proj_recv, own_sem,
):
    me = lax.axis_index("dev")
    low = list(range(unit))
    mates = [flipped(me, subset(low, number)) for number in range(1, 1 << unit)]
    ranks = [flipped(me, [unit + bit]) for bit in bits]
    barrier = pltpu.get_barrier_semaphore()
    for other in mates + ranks:
        pl.semaphore_signal(barrier, inc=1, device_id={"dev": other}, device_id_type=MESH)
    request = me % (1 << unit)
    rank = me // (1 << unit)
    parity = rank % 2
    depth = proj_ref.shape[0]
    own_rows = pl.ds(pl.multiple_of(request * depth, depth), depth)
    own_half = pltpu.make_async_copy(kv_ref, halves.at[parity], own_sem.at[0])
    own_proj = pltpu.make_async_copy(proj_ref, proj.at[own_rows], own_sem.at[1])
    own_half.start()
    own_proj.start()
    pl.semaphore_wait(barrier, len(mates) + len(ranks))
    kv_copy = pltpu.make_async_remote_copy(
        src_ref=kv_ref,
        dst_ref=halves.at[parity],
        send_sem=kv_sem.at[0],
        recv_sem=kv_sem.at[1],
        device_id={"dev": ranks[0]},
        device_id_type=MESH,
    )
    kv_copy.start()
    proj_copies = []
    for place, other in enumerate(mates):
        copy = pltpu.make_async_remote_copy(
            src_ref=proj_ref,
            dst_ref=proj.at[own_rows],
            send_sem=proj_send.at[place],
            recv_sem=proj_recv.at[place],
            device_id={"dev": other},
            device_id_type=MESH,
        )
        copy.start()
        proj_copies.append(copy)
    own_half.wait()
    kv_copy.wait()

    blocks, rows, width = x.shape
    far = 1 << (len(bits) - 1)
    masks = sorted(range(blocks), key=lambda m: (-bin(m).count("1"), -(m & far), m))
    place_of = {mask: place for place, mask in enumerate(masks)}
    length = lengths_ref[request]
    runs = [
        scatter_steps(
            me, unit, number, order, cols, x, recv, stage, send_sem, recv_sem,
            lambda flips: place_of[sum(1 << bit for bit in flips)],
        )
        for number, (order, cols) in enumerate(parts)
    ]
    half = blocks // 2
    strip = math.gcd(width, 512)
    for group in range(2):
        for spot in range(half):
            mask = masks[group * half + spot]
            block = flipped(rank, subset(bits, mask))
            heads[spot * rows : (spot + 1) * rows, :] = attend_block(
                block, length, q_ref, halves, rows
            )
        if group == 0:
            own_proj.wait()
            for copy in proj_copies:
                copy.wait()
        for start in range(0, width, strip):
            product = jnp.dot(
                heads[...], proj[:, start : start + strip], preferred_element_type=jnp.float32
            ).astype(x.dtype)
            for spot in range(half):
                x[group * half + spot, :, start : start + strip] = product[
                    spot * rows : (spot + 1) * rows
                ]
        for spot in range(half):
            mask = masks[group * half + spot]
            for (send, _), (order, _) in zip(runs, parts):
                if mask >> order[0] & 1:
                    number = sum((mask >> bit & 1) << at for at, bit in enumerate(order[1:]))
                    send(0, number)
    for step in range(1, len(bits)):
        for send, _ in runs:
            send(step)
    for _, finish in runs:
        finish(o_ref)


def attention(lengths, queries, key_values, out_proj, unit, orders, collective_id):
    width = out_proj.shape[1]
    tokens, columns = queries.shape
    bits = sorted(orders[0])
    blocks = 1 << len(bits)
    rows = tokens // blocks
    cut = width * 3 // 4 // 128 * 128
    parts = [(orders[0], pl.ds(0, cut)), (orders[1], pl.ds(cut, width - cut))]
    mates = max((1 << unit) - 1, 1)
    kind = queries.dtype
    whole = pl.BlockSpec(memory_space=pltpu.VMEM)
    return pl.pallas_call(
        functools.partial(attention_kernel, unit, parts, bits),
        out_shape=jax.ShapeDtypeStruct((rows, width), jnp.float32),
        in_specs=[pl.BlockSpec(memory_space=pltpu.SMEM), whole, whole, whole],
        out_specs=whole,
        scratch_shapes=[
            pltpu.VMEM((2,) + key_values.shape, kind),
            pltpu.VMEM((out_proj.shape[0] << unit, width), kind),
            pltpu.VMEM((tokens // 2, columns), kind),
            pltpu.VMEM((blocks, rows, width), kind),
            pltpu.VMEM((blocks - 1, rows, width), kind),
            pltpu.VMEM((max(blocks // 2 - 1, 1), rows, width), kind),
            pltpu.SemaphoreType.DMA((2, blocks - 1)),
            pltpu.SemaphoreType.DMA((2, blocks - 1)),
            pltpu.SemaphoreType.DMA((2,)),
            pltpu.SemaphoreType.DMA((mates,)),
            pltpu.SemaphoreType.DMA((mates,)),
            pltpu.SemaphoreType.DMA((2,)),
        ],
        compiler_params=pltpu.CompilerParams(collective_id=collective_id, has_side_effects=True),
    )(lengths, queries, key_values, out_proj)


def reduce_scatter(x, unit, orders, collective_id):
    blocks, rows, width = x.shape
    bits = sorted(orders[0])
    cut = width * 3 // 4 // 128 * 128
    parts = [(orders[0], pl.ds(0, cut)), (orders[1], pl.ds(cut, width - cut))]
    return pl.pallas_call(
        functools.partial(scatter_kernel, unit, parts, bits),
        out_shape=jax.ShapeDtypeStruct((rows, width), jnp.float32),
        in_specs=[pl.BlockSpec(memory_space=pltpu.VMEM)],
        out_specs=pl.BlockSpec(memory_space=pltpu.VMEM),
        scratch_shapes=[
            pltpu.VMEM((blocks - 1, rows, width), x.dtype),
            pltpu.VMEM((max(blocks // 2 - 1, 1), rows, width), x.dtype),
            pltpu.SemaphoreType.DMA((2, blocks - 1)),
            pltpu.SemaphoreType.DMA((2, blocks - 1)),
        ],
        compiler_params=pltpu.CompilerParams(collective_id=collective_id, has_side_effects=True),
    )(x)


def gather_kernel(parts, bits, x_ref, g_ref, ox_ref, og_ref, send_sem, recv_sem, own_sem):
    me = lax.axis_index("dev")
    greet(me, bits)
    k = len(bits)
    pairs = [(x_ref, ox_ref), (g_ref, og_ref)]
    local = []
    for number, (source, target) in enumerate(pairs):
        copy = pltpu.make_async_copy(source, target.at[me], own_sem.at[number])
        copy.start()
        local.append(copy)
    sent = []

    def forward(part_no, held, step):
        which, order, cols = parts[part_no]
        source, target = pairs[which]
        block = flipped(me, subset(order, held))
        slot = (1 << step) - 1 + held
        copy = pltpu.make_async_remote_copy(
            src_ref=source.at[:, cols] if held == 0 else target.at[block, :, cols],
            dst_ref=target.at[block, :, cols],
            send_sem=send_sem.at[part_no, slot],
            recv_sem=recv_sem.at[part_no, slot],
            device_id={"dev": flipped(me, [order[step]])},
            device_id_type=MESH,
        )
        copy.start()
        sent.append(copy)

    def arrive(part_no, held, step):
        which, order, cols = parts[part_no]
        target = pairs[which][1]
        block = flipped(me, subset(order, held) + [order[step]])
        slot = (1 << step) - 1 + held
        pltpu.make_async_remote_copy(
            src_ref=target.at[block, :, cols],
            dst_ref=target.at[block, :, cols],
            send_sem=send_sem.at[part_no, slot],
            recv_sem=recv_sem.at[part_no, slot],
            device_id={"dev": flipped(me, [order[step]])},
            device_id_type=MESH,
        ).wait_recv()

    for step in range(k):
        for part_no in range(len(parts)):
            forward(part_no, 0, step)
    for step in range(k):
        for held in range(1 << step):
            for part_no in range(len(parts)):
                arrive(part_no, held, step)
                for later in range(step + 1, k):
                    forward(part_no, held + (1 << step), later)
    for copy in local:
        copy.wait()
    for copy in sent:
        copy.wait_send()


def all_gather(x, gates, orders, collective_id):
    rows, width = x.shape
    bits = sorted(orders[0])
    count = 1 << len(bits)
    cut = width * 3 // 4 // 128 * 128
    parts = [
        (1, orders[0], pl.ds(0, gates.shape[1])),
        (0, orders[0], pl.ds(0, cut)),
        (0, orders[1], pl.ds(cut, width - cut)),
    ]
    return pl.pallas_call(
        functools.partial(gather_kernel, parts, bits),
        out_shape=[
            jax.ShapeDtypeStruct((count, rows, width), x.dtype),
            jax.ShapeDtypeStruct((count,) + gates.shape, gates.dtype),
        ],
        in_specs=[pl.BlockSpec(memory_space=pltpu.VMEM)] * 2,
        out_specs=[pl.BlockSpec(memory_space=pltpu.VMEM)] * 2,
        scratch_shapes=[
            pltpu.SemaphoreType.DMA((3, count - 1)),
            pltpu.SemaphoreType.DMA((3, count - 1)),
            pltpu.SemaphoreType.DMA((2,)),
        ],
        compiler_params=pltpu.CompilerParams(collective_id=collective_id, has_side_effects=True),
    )(x, gates)


def swapped(order, one, two):
    order = list(order)
    order[one], order[two] = order[two], order[one]
    return order


def per_device(
    queries,
    key_values,
    lengths,
    out_proj,
    residual,
    norm_gain,
    router,
    expert_ids,
    expert_gate_up,
    expert_down,
):
    devices = lax.axis_size("dev")
    my_index = lax.axis_index("dev")
    width = residual.shape[-1]
    requests_n = devices // GROUP
    low_bits = bit_count(requests_n)
    near = list(range(bit_count(GROUP)))
    attended = attention(
        lengths, queries[0], key_values[:, 0], out_proj, low_bits, [near, swapped(near, 0, 1)], 1
    )
    stream = (residual[0].astype(jnp.float32) + attended).astype(jnp.bfloat16)
    values = stream.astype(jnp.float32)
    normed = (
        values
        * lax.rsqrt(jnp.mean(values * values, axis=-1, keepdims=True) + EPSILON)
        * norm_gain.astype(jnp.float32)
    ).astype(jnp.bfloat16)
    logits = jnp.dot(normed, router, preferred_element_type=jnp.float32)
    experts_n = router.shape[1]
    token_ids = expert_ids[0]
    named = jnp.any(token_ids[..., None] == jnp.arange(experts_n, dtype=jnp.int32), axis=1)
    raised_gate = jnp.where(named, jnp.exp(logits), 0.0)
    gates = raised_gate / jnp.sum(raised_gate, axis=-1, keepdims=True)
    lanes = -(-TOK_DEV // 128) * 128
    gates = jnp.pad(gates.T, ((0, 0), (0, lanes - TOK_DEV)))
    every = list(range(bit_count(devices)))
    far = every[::-1]
    count = len(far)
    rows_all, gates_all = all_gather(normed, gates, [far, swapped(far, count - 3, count - 2)], 2)
    my_gates = lax.dynamic_index_in_dim(gates_all, my_index, 1, keepdims=False)[:, :TOK_DEV]
    flat_rows = rows_all.reshape(devices * TOK_DEV, width)
    projected = jnp.dot(flat_rows, expert_gate_up[0], preferred_element_type=jnp.float32)
    activation = (jax.nn.silu(projected[:, :FF]) * projected[:, FF:]).astype(jnp.bfloat16)
    produced = jnp.dot(activation, expert_down[0], preferred_element_type=jnp.float32)
    weighted = (my_gates.reshape(-1, 1) * produced).astype(jnp.bfloat16)
    weighted = weighted.reshape(devices, TOK_DEV, width)
    combined = reduce_scatter(weighted, 0, [every, swapped(every, 1, 2)], 3)
    return (values + combined).astype(jnp.bfloat16)[None]


def solution(mesh):
    return jax.shard_map(
        per_device,
        mesh=mesh,
        in_specs=(
            P(("groups", "dev"), None, None),
            P(None, ("groups", "dev"), None, None),
            P("groups"),
            P("dev", None),
            P(("groups", "dev"), None, None),
            P(),
            P(),
            P(("groups", "dev"), None, None),
            P("dev", None, None),
            P("dev", None, None),
        ),
        out_specs=P(("groups", "dev"), None, None),
        check_vma=False,
    )
```
